32 devices in a mesh: section: 8 (over y, x, core), tensor: 4 (over z).
Axes of the slice: x: 2, y: 2, z: 4, core: 2. Of those that a mesh axis runs over, the one named last changes fastest.
Arguments:
- arriving: bfloat16 [8, 512, 16384], P('section', 'tensor'), may hold values from -6 to 6
- kept_input: bfloat16 [8, 512, 16384], P('section', 'tensor'), may hold values from -6 to 6
- returning: bfloat16 [8, 512, 16384], P('section', 'tensor'), may hold values from -6 to 6
- norm_gain: bfloat16 [8, 16384], P('section'), may hold values from 0.25 to 1.75
- key_weight: bfloat16 [8, 16384, 1024], P('section', 'tensor'), may hold values from -0.0625 to 0.0625
- value_weight: bfloat16 [8, 16384, 1024], P('section', 'tensor'), may hold values from -0.0625 to 0.0625
- key_down: bfloat16 [8, 16384, 16], P('section', 'tensor'), may hold values from -0.046875 to 0.046875
- value_down: bfloat16 [8, 16384, 16], P('section', 'tensor'), may hold values from -0.046875 to 0.046875
- key_up: bfloat16 [8, 16, 1024], P('section', None, 'tensor'), may hold values from -1.5 to 1.5
- value_up: bfloat16 [8, 16, 1024], P('section', None, 'tensor'), may hold values from -1.5 to 1.5
- key_cot: bfloat16 [8, 512, 1024], P('section', None, 'tensor'), may hold values from -6 to 6
- value_cot: bfloat16 [8, 512, 1024], P('section', None, 'tensor'), may hold values from -6 to 6
Outputs:
- keys: bfloat16 [8, 512, 1024], P('section', None, 'tensor')
- values: bfloat16 [8, 512, 1024], P('section', None, 'tensor')
- input_grad: bfloat16 [8, 512, 16384], P('section', 'tensor')
- key_down_grad: float32 [8, 16384, 16], P('section', 'tensor')
- value_down_grad: float32 [8, 16384, 16], P('section', 'tensor')
- key_up_grad: float32 [8, 16, 1024], P('section', None, 'tensor')
- value_up_grad: float32 [8, 16, 1024], P('section', None, 'tensor')
The draws below stay inside these ranges and needn't reach their ends.
All inputs are finite; a program needn't handle non-finite values.
Results may differ from the reference program's by a relative error of at most 0.014.
Values may be sent and summed in bfloat16 or wider, within the bound.
A program may use at most 192 MiB of HBM per device.

```python
import jax
import jax.numpy as jnp
from jax import lax

D = 16384
RANK = 16
TOKENS = 512
KVW = 1024
LAYERS = 8


def with_spikes(values, stream_key, source, target, blocks, factor):
    def block_of(position):
        return (jnp.arange(values.shape[position]) // (values.shape[position] // blocks)).reshape((-1,) + (1,) * (values.ndim - 1 - position))

    one_side = jax.random.permutation(stream_key, blocks)[block_of(target)]
    other_side = (block_of(target) + blocks // 2) % blocks
    return jnp.where((block_of(source) == one_side) | (block_of(source) == other_side), factor * values, values)


def block_scale(stream_key, dims, cuts, low, high):
    level = 1.0
    for position, shards_of in cuts:
        draws = jax.random.uniform(jax.random.fold_in(jax.random.fold_in(stream_key, 6), position), (shards_of,), jnp.float32, low / len(cuts), high / len(cuts))
        level = level * jnp.repeat(jnp.exp(draws), dims[position] // shards_of).reshape((-1,) + (1,) * (len(dims) - 1 - position))
    return level


def bell_draw(key, extent, scale, reach, shards=(), held_as=jnp.bfloat16):
    factor_of = block_scale(key, extent, shards, -0.22, 0.18) if shards else 1.0
    result = jax.random.normal(key, extent, jnp.float32) * scale * factor_of
    return jnp.minimum(jnp.maximum(result, -reach), reach).astype(held_as)


def noise_with(stream_key, extent, spread, bound, pieces, heavy, dtype=jnp.bfloat16):
    entries = spread * jax.random.normal(stream_key, extent, jnp.float32)
    if pieces:
        entries = entries * block_scale(stream_key, extent, pieces, -0.22, 0.18)
    return jnp.clip(with_spikes(entries, jax.random.fold_in(stream_key, 3), *heavy), -bound, bound).astype(dtype)


def setup_inputs(seed: int = 0) -> dict:
    key_of = jax.random.split(jax.random.key(seed), 13)
    return {
        "arriving": bell_draw(key_of[0], (LAYERS, TOKENS, D), 1.0, 6.0, ((0, 8), (1, 4))),
        "kept_input": bell_draw(key_of[1], (LAYERS, TOKENS, D), 1.0, 6.0, ((0, 8), (1, 4))),
        "returning": bell_draw(key_of[2], (LAYERS, TOKENS, D), 1.0, 6.0, ((0, 8), (1, 4))),
        "norm_gain": jnp.clip(1.0 + 0.15 * jax.random.normal(key_of[3], (LAYERS, D), jnp.float32), 0.25, 1.75).astype(jnp.bfloat16),
        "key_weight": noise_with(key_of[4], (LAYERS, D, KVW), D ** -0.5, 0.0625, ((0, 8), (1, 4)), (1, 2, 4, 2.0)),
        "value_weight": noise_with(key_of[5], (LAYERS, D, KVW), D ** -0.5, 0.0625, ((0, 8), (1, 4)), (1, 2, 4, 2.0)),
        "key_down": bell_draw(key_of[6], (LAYERS, D, RANK), D ** -0.5, 0.046875, ((0, 8), (1, 4))),
        "value_down": bell_draw(key_of[7], (LAYERS, D, RANK), D ** -0.5, 0.046875, ((0, 8), (1, 4))),
        "key_up": bell_draw(key_of[8], (LAYERS, RANK, KVW), RANK ** -0.5, 1.5, ((0, 8), (2, 4))),
        "value_up": bell_draw(key_of[9], (LAYERS, RANK, KVW), RANK ** -0.5, 1.5, ((0, 8), (2, 4))),
        "key_cot": bell_draw(key_of[10], (LAYERS, TOKENS, KVW), 1.0, 6.0, ((0, 8), (2, 4))),
        "value_cot": bell_draw(key_of[11], (LAYERS, TOKENS, KVW), 1.0, 6.0, ((0, 8), (2, 4))),
    }


epsilon = 1e-05
adapter_scale = 2.0

def normalize(hidden, gain):
    values = hidden.astype(jnp.float32)
    inverse = lax.rsqrt(lax.optimization_barrier(jnp.mean(values * values, axis=-1, keepdims=True)) + epsilon)
    return (inverse, (values * inverse * gain.astype(jnp.float32)).astype(jnp.bfloat16))

def precise_product(left, right):
    return jnp.dot(left, right, precision=lax.Precision.HIGHEST, preferred_element_type=jnp.float32)

def mixed_product(left, right):
    return jnp.dot(left.astype(jnp.float32), right.astype(jnp.float32), preferred_element_type=jnp.float32)

def one_layer(blocks):
    incoming, kept, back, gain, key_matrix, value_matrix, key_down_matrix, value_down_matrix, key_up_matrix, value_up_matrix, key_cotangent, value_cotangent = blocks
    _, normed_input = normalize(incoming, gain)
    key_middle = mixed_product(normed_input, key_down_matrix)
    value_middle = mixed_product(normed_input, value_down_matrix)
    keys = (mixed_product(normed_input, key_matrix) + adapter_scale * precise_product(key_middle, key_up_matrix.astype(jnp.float32))).astype(jnp.bfloat16)
    values = (mixed_product(normed_input, value_matrix) + adapter_scale * precise_product(value_middle, value_up_matrix.astype(jnp.float32))).astype(jnp.bfloat16)
    adapted_key = mixed_product(key_cotangent, key_up_matrix.T)
    adapted_value = mixed_product(value_cotangent, value_up_matrix.T)
    branch_output = mixed_product(key_cotangent, key_matrix.T) + mixed_product(value_cotangent, value_matrix.T)
    branch_output = branch_output + adapter_scale * (precise_product(adapted_key, key_down_matrix.T.astype(jnp.float32)) + precise_product(adapted_value, value_down_matrix.T.astype(jnp.float32)))
    branch_output = lax.optimization_barrier(branch_output.astype(jnp.bfloat16)).astype(jnp.float32)
    inverse, kept_normed = normalize(kept, gain)
    kept_values = kept.astype(jnp.float32)
    scaled = gain.astype(jnp.float32) * branch_output
    inner = lax.optimization_barrier(jnp.mean(kept_values * scaled, axis=-1, keepdims=True))
    input_grad = (back.astype(jnp.float32) + inverse * scaled - kept_values * inverse * inverse * inverse * inner).astype(jnp.bfloat16)
    saved_wide_input = kept_normed.astype(jnp.float32)
    key_down_gradient = adapter_scale * precise_product(saved_wide_input.T, adapted_key)
    value_down_gradient = adapter_scale * precise_product(saved_wide_input.T, adapted_value)
    key_middle_rows = mixed_product(kept_normed, key_down_matrix)
    value_middle_rows = mixed_product(kept_normed, value_down_matrix)
    key_up_gradient = adapter_scale * precise_product(key_middle_rows.T, key_cotangent.astype(jnp.float32))
    value_up_gradient = adapter_scale * precise_product(value_middle_rows.T, value_cotangent.astype(jnp.float32))
    return (keys, values, input_grad, key_down_gradient, value_down_gradient, key_up_gradient, value_up_gradient)

def reference(arriving, kept_input, returning, norm_gain, key_weight, value_weight, key_down, value_down, key_up, value_up, key_cot, value_cot):
    incoming = jnp.roll(arriving, 1, axis=0)
    back = jnp.roll(returning, -1, axis=0)
    layer_count = arriving.shape[0]
    collected = []
    for layer in range(layer_count):
        blocks = (incoming[layer], kept_input[layer], back[layer], norm_gain[layer], key_weight[layer], value_weight[layer], key_down[layer], value_down[layer], key_up[layer], value_up[layer], key_cot[layer], value_cot[layer])
        collected.append(one_layer(blocks))
    stacked = [jnp.stack([item[index] for item in collected], axis=0) for index in range(7)]
    return (stacked[0], stacked[1], stacked[2], stacked[3], stacked[4], stacked[5], stacked[6])
```

```python
import functools

import jax
import jax.numpy as jnp
from jax import lax
from jax.experimental import pallas as pl
from jax.experimental.pallas import tpu as pltpu
from jax.sharding import PartitionSpec as P

epsilon = 1e-05
adapter_scale = 2.0
bf16 = jnp.bfloat16
f32 = jnp.float32


def shift(x, axis, by):
    count = lax.axis_size(axis)
    return lax.ppermute(x, axis, [(i, (i + by) % count) for i in range(count)])


def swap(x, bit):
    count = lax.axis_size("tensor")
    return lax.ppermute(x, "tensor", [(i, i ^ bit) for i in range(count)])


def bits_up():
    count = lax.axis_size("tensor")
    bits = []
    bit = 1
    while bit < count:
        bits.append(bit)
        bit *= 2
    return bits


def gather_blocks(x, far_first):
    me = lax.axis_index("tensor")
    held = x[None]
    for bit in reversed(bits_up()) if far_first else bits_up():
        other = swap(held, bit)
        upper = (me & bit) != 0
        pair = jnp.stack(
            [jnp.where(upper, other, held), jnp.where(upper, held, other)],
            axis=1 if far_first else 0,
        )
        held = pair.reshape((2 * held.shape[0],) + x.shape)
    return held


def scatter_sum(x, far_first):
    me = lax.axis_index("tensor")
    for bit in reversed(bits_up()) if far_first else bits_up():
        mine = (me // bit) % 2
        half = x.shape[0] // 2
        axis = 0 if far_first else 1
        pairs = x.reshape(((2, half) if far_first else (half, 2)) + x.shape[1:])
        give = lax.dynamic_index_in_dim(pairs, 1 - mine, axis, keepdims=False)
        keep = lax.dynamic_index_in_dim(pairs, mine, axis, keepdims=False)
        got = swap(give.astype(bf16), bit)
        x = keep.astype(f32) + got.astype(f32)
        if x.shape[0] > 1:
            x = x.astype(bf16)
    return x[0]


def norm_kernel(count, x_ref, gain_ref, out_ref):
    width = x_ref.shape[1] // count
    x = x_ref[...].astype(f32)
    inverse = lax.rsqrt(jnp.mean(x * x, axis=-1, keepdims=True) + epsilon)
    for j in range(count):
        cols = slice(j * width, (j + 1) * width)
        part = x_ref[:, cols].astype(f32) * inverse * gain_ref[:, cols].astype(f32)
        out_ref[j] = part.astype(bf16)


def norm_split(x, gain, count):
    rows, width = x.shape
    tile = 16
    return pl.pallas_call(
        functools.partial(norm_kernel, count),
        grid=(rows // tile,),
        in_specs=[
            pl.BlockSpec((tile, width), lambda i: (i, 0)),
            pl.BlockSpec((1, width), lambda i: (0, 0)),
        ],
        out_specs=pl.BlockSpec((count, tile, width // count), lambda i: (0, i, 0)),
        out_shape=jax.ShapeDtypeStruct((count, rows, width // count), bf16),
        cost_estimate=pl.CostEstimate(
            flops=6 * rows * width, bytes_accessed=4 * rows * width, transcendentals=0
        ),
    )(x, gain)


def dot_nt(a, b):
    return lax.dot_general(a, b, (((1,), (1,)), ((), ())), preferred_element_type=f32)


def head_kernel(count, me_ref, *refs):
    x_refs = refs[:count]
    wk_ref, wv_ref, down_ref, up_ref, out_ref, mid_ref = refs[count:]
    rank = down_ref.shape[0] // 2
    rows = x_refs[0].shape[0]

    @pl.when(pl.program_id(0) == 0)
    def _():
        for j in range(count):
            for s in range(2):
                mid = dot_nt(x_refs[j][...], down_ref[s * rank : (s + 1) * rank, :])
                mid_ref[s, j * rows : (j + 1) * rows, :] = (adapter_scale * mid).astype(bf16)

    for j in range(count):
        start = pl.multiple_of((me_ref[0] ^ j) * rows, rows)
        for s, w_ref in enumerate((wk_ref, wv_ref)):
            total = jnp.dot(x_refs[j][...], w_ref[...], preferred_element_type=f32)
            up = up_ref[0, s * rank : (s + 1) * rank, :]
            mid = mid_ref[s, j * rows : (j + 1) * rows, :]
            total = total + jnp.dot(mid, up, preferred_element_type=f32)
            out_ref[0, s, pl.ds(start, rows), :] = total.astype(bf16)


def head_sums(blocks, wk, wv, down, ups):
    rows, depth = blocks[0].shape
    count, twice, heads = ups.shape
    tokens = rows * count
    me = lax.axis_index("tensor").astype(jnp.int32).reshape(1)
    return pl.pallas_call(
        functools.partial(head_kernel, count),
        grid=(count,),
        in_specs=[pl.BlockSpec(memory_space=pltpu.SMEM)]
        + [pl.BlockSpec((rows, depth), lambda i: (0, 0))] * count
        + [
            pl.BlockSpec((depth, heads), lambda i: (0, i)),
            pl.BlockSpec((depth, heads), lambda i: (0, i)),
            pl.BlockSpec((twice, depth), lambda i: (0, 0)),
            pl.BlockSpec((1, twice, heads), lambda i: (i, 0, 0)),
        ],
        out_specs=pl.BlockSpec((1, 2, tokens, heads), lambda i: (i, 0, 0, 0)),
        out_shape=jax.ShapeDtypeStruct((count, 2, tokens, heads), bf16),
        scratch_shapes=[pltpu.VMEM((2, tokens, twice // 2), bf16)],
        compiler_params=pltpu.CompilerParams(vmem_limit_bytes=48 * 2**20),
        cost_estimate=pl.CostEstimate(
            flops=4 * tokens * depth * heads * count,
            bytes_accessed=4 * depth * heads * count,
            transcendentals=0,
        ),
    )(me, *blocks, wk, wv, down, ups)


def branch_kernel(tokens, cot_ref, wk_ref, wv_ref, down_ref, out_ref, adk_ref, adv_ref):
    count, _, heads = cot_ref.shape
    rank = down_ref.shape[0] // 2
    ad_refs = (adk_ref, adv_ref)

    @pl.when(pl.program_id(0) == 0)
    def _():
        for s in range(2):
            total = jnp.zeros((tokens, rank), f32)
            for j in range(count):
                up = cot_ref[j, 2 * tokens + s * rank : 2 * tokens + (s + 1) * rank, :]
                total = total + dot_nt(cot_ref[j, s * tokens : (s + 1) * tokens, :], up)
            ad_refs[s][...] = total

    total = jnp.zeros(out_ref.shape, f32)
    for s, w_ref in enumerate((wk_ref, wv_ref)):
        ad = (adapter_scale * ad_refs[s][...]).astype(bf16)
        down = down_ref[s * rank : (s + 1) * rank, :]
        total = total + jnp.dot(ad, down, preferred_element_type=f32)
        for j in range(count):
            total = total + dot_nt(
                cot_ref[j, s * tokens : (s + 1) * tokens, :],
                w_ref[:, j * heads : (j + 1) * heads],
            )
    out_ref[...] = total.astype(bf16)


def branch_block(cots, wk, wv, down, tokens):
    count, rows, heads = cots.shape
    depth, wide = wk.shape
    twice = down.shape[0]
    tile = min(512, depth)
    return pl.pallas_call(
        functools.partial(branch_kernel, tokens),
        grid=(depth // tile,),
        in_specs=[
            pl.BlockSpec((count, rows, heads), lambda i: (0, 0, 0)),
            pl.BlockSpec((tile, wide), lambda i: (i, 0)),
            pl.BlockSpec((tile, wide), lambda i: (i, 0)),
            pl.BlockSpec((twice, tile), lambda i: (0, i)),
        ],
        out_specs=[
            pl.BlockSpec((tokens, tile), lambda i: (0, i)),
            pl.BlockSpec((tokens, twice // 2), lambda i: (0, 0)),
            pl.BlockSpec((tokens, twice // 2), lambda i: (0, 0)),
        ],
        out_shape=[
            jax.ShapeDtypeStruct((tokens, depth), bf16),
            jax.ShapeDtypeStruct((tokens, twice // 2), f32),
            jax.ShapeDtypeStruct((tokens, twice // 2), f32),
        ],
        compiler_params=pltpu.CompilerParams(vmem_limit_bytes=48 * 2**20),
        cost_estimate=pl.CostEstimate(
            flops=4 * tokens * depth * wide, bytes_accessed=4 * depth * wide, transcendentals=0
        ),
    )(cots, wk, wv, down)


def grad_kernel(branch_ref, kept_ref, back_ref, gain_ref, out_ref):
    count, _, width = branch_ref.shape
    tile, total = kept_ref.shape
    squares = jnp.zeros((tile, 1), f32)
    inner = jnp.zeros((tile, 1), f32)
    for j in range(count):
        cols = slice(j * width, (j + 1) * width)
        h = kept_ref[:, cols].astype(f32)
        scaled = gain_ref[:, cols].astype(f32) * branch_ref[j].astype(f32)
        squares = squares + jnp.sum(h * h, axis=-1, keepdims=True)
        inner = inner + jnp.sum(h * scaled, axis=-1, keepdims=True)
    inverse = lax.rsqrt(squares / total + epsilon)
    pull = inverse * inverse * inverse * (inner / total)
    for j in range(count):
        cols = slice(j * width, (j + 1) * width)
        h = kept_ref[:, cols].astype(f32)
        scaled = gain_ref[:, cols].astype(f32) * branch_ref[j].astype(f32)
        value = back_ref[:, cols].astype(f32) + inverse * scaled - h * pull
        out_ref[:, cols] = value.astype(bf16)


def grad_rows(branch, kept, back, gain):
    count, rows, width = branch.shape
    total = kept.shape[1]
    tile = 16
    row_spec = pl.BlockSpec((tile, total), lambda i: (i, 0))
    return pl.pallas_call(
        grad_kernel,
        grid=(rows // tile,),
        in_specs=[
            pl.BlockSpec((count, tile, width), lambda i: (0, i, 0)),
            row_spec,
            row_spec,
            pl.BlockSpec((1, total), lambda i: (0, 0)),
        ],
        out_specs=row_spec,
        out_shape=jax.ShapeDtypeStruct((rows, total), bf16),
        cost_estimate=pl.CostEstimate(
            flops=12 * rows * total, bytes_accessed=8 * rows * total, transcendentals=0
        ),
    )(branch, kept, back, gain)


def exchange(x):
    return lax.all_to_all(x, "tensor", split_axis=0, concat_axis=0, tiled=True)


def on_device(
    arriving,
    kept_input,
    returning,
    norm_gain,
    key_weight,
    value_weight,
    key_down,
    value_down,
    key_up,
    value_up,
    key_cot,
    value_cot,
):
    count = lax.axis_size("tensor")
    kept = kept_input[0]
    rows, width = kept.shape
    tokens = key_cot.shape[1]
    rank = key_up.shape[1]
    depth = width // count

    next_gain = shift(norm_gain, "section", -1)
    cots = gather_blocks(
        jnp.concatenate([key_cot[0], value_cot[0], key_up[0], value_up[0]], axis=0), True
    )
    down = jnp.concatenate([key_down[0].T, value_down[0].T], axis=0)
    down_blocks = gather_blocks(down, False)
    back = shift(returning, "section", -1)[0]
    normed = norm_split(arriving[0], next_gain, count)
    normed, cots, down_blocks = lax.optimization_barrier((normed, cots, down_blocks))
    me = lax.axis_index("tensor")
    spread = [None] * count
    for j in (0,) + tuple(reversed(range(1, count))):
        block = lax.dynamic_index_in_dim(normed, me ^ j, 0, keepdims=False)
        spread[j] = swap(block, j) if j else block

    branch, adapt_key, adapt_value = branch_block(
        cots, key_weight[0], value_weight[0], down, tokens
    )
    branch_rows = exchange(branch.reshape(count, rows, depth))
    spread = [shift(block, "section", 1) for block in spread]

    kept_split = norm_split(kept, norm_gain, count)
    offset = lax.axis_index("tensor") * rows
    adapt = jnp.concatenate([adapt_key, adapt_value], axis=1)
    mine = lax.dynamic_slice_in_dim(adapt, offset, rows, 0)
    down_parts = jnp.einsum(
        "tr,jtd->jrd", (adapter_scale * mine).astype(bf16), kept_split,
        preferred_element_type=f32,
    ).astype(bf16)
    middle = jnp.einsum("jtd,jrd->tr", kept_split, down_blocks, preferred_element_type=f32)
    middle = (adapter_scale * middle).astype(bf16)
    up_parts = jnp.concatenate(
        [
            jnp.einsum(
                "tr,jth->jrh",
                middle[:, s * rank : (s + 1) * rank],
                lax.dynamic_slice_in_dim(cots, offset + s * tokens, rows, 1),
                preferred_element_type=f32,
            )
            for s in range(2)
        ],
        axis=1,
    )
    parts = jnp.concatenate([down_parts, up_parts.astype(bf16)], axis=2)

    sums = head_sums(spread, key_weight[0], value_weight[0], down, cots[:, 2 * tokens :])
    sums, parts = lax.optimization_barrier((sums, parts))
    parts, branch_rows = lax.optimization_barrier((parts, branch_rows))
    grads = scatter_sum(parts, True)
    heads = scatter_sum(sums, False).astype(bf16)
    down_grad, up_grad = grads[:, :depth], grads[:, depth:]
    input_grad = grad_rows(branch_rows, kept, back, norm_gain)
    return (
        heads[0][None],
        heads[1][None],
        input_grad[None],
        down_grad[:rank].T[None],
        down_grad[rank:].T[None],
        up_grad[:rank][None],
        up_grad[rank:][None],
    )


def solution(mesh):
    return jax.shard_map(
        on_device,
        mesh=mesh,
        in_specs=(
            P("section", "tensor", None),
            P("section", "tensor", None),
            P("section", "tensor", None),
            P("section", None),
            P("section", "tensor", None),
            P("section", "tensor", None),
            P("section", "tensor", None),
            P("section", "tensor", None),
            P("section", None, "tensor"),
            P("section", None, "tensor"),
            P("section", None, "tensor"),
            P("section", None, "tensor"),
        ),
        out_specs=(
            P("section", None, "tensor"),
            P("section", None, "tensor"),
            P("section", "tensor", None),
            P("section", "tensor", None),
            P("section", "tensor", None),
            P("section", None, "tensor"),
            P("section", None, "tensor"),
        ),
        check_vma=False,
    )
```
